256 devices in a mesh: stream: 32 (over y_hi, z, core), tm: 8 (over x, y_lo).
Axes of the slice: x: 4, y: 4 (y_hi: 2, y_lo: 2; y = y_hi * 2 + y_lo), z: 8, core: 2. Of those that a mesh axis runs over, the one named last changes fastest.
Arguments:
- signal: bfloat16 [64, 2, 4194304], P('stream', None, 'tm'), parts along dimension 0, may hold values from -11 to 11
- taps: float32 [16, 4096], replicated, may hold values from -1.5 to 1.5
Outputs:
- channels_out: float32 [64, 2, 4096, 1024], P('stream', None, 'tm'), parts along dimension 0
The draws below stay inside these ranges and needn't reach their ends.
There are 32 independent parts, one for each index of `stream`. The reference program is written for one: setup_inputs(seed, part) draws one part's arguments, and reference() takes and returns one part's arrays. A program takes and returns all parts, laid end to end along the dimension named above; an argument that names none is the same for every part. Nothing has to cross between parts.
All inputs are finite; a program needn't handle non-finite values.
Results may differ from the reference program's by a relative error of at most 0.0003.
Values may be sent and summed in bfloat16 or wider, within the bound.
No kernel may reach another device: no remote copies, remote signals or barrier semaphores. Data moves between devices by JAX's collectives and lax.ppermute only.
A program may use at most 128 MiB of HBM per device.

```python
import math
import jax
import jax.numpy as jnp
from jax import lax

CHANNELS = 4096
RADIX = 64
TAPS = 16
STREAMS = 2
FRAMES = 1024
SAMPLES = 4194304


def draw_signal(key, part):
    key_noise, key_gain, key_freq, key_level = jax.random.split(key, 4)
    blocks = FRAMES // 8 + 1
    position = jnp.arange(SAMPLES, dtype=jnp.int32)
    which = position // CHANNELS // 8
    noise = jax.random.truncated_normal(key_noise, -4.0, 4.0, (STREAMS, 2, SAMPLES), jnp.float32)
    gains = jnp.exp(jax.random.uniform(key_gain, (STREAMS, blocks), jnp.float32, math.log(0.5), math.log(2.0)))
    envelope = gains[:, which]
    numerators = jax.random.randint(key_freq, (STREAMS, 3), 0, 1 << 20, jnp.int32)
    levels = jax.random.uniform(key_level, (STREAMS, 3), jnp.float32, 0.3, 1.0)
    tone_real = jnp.zeros((STREAMS, SAMPLES), jnp.float32)
    tone_imag = jnp.zeros((STREAMS, SAMPLES), jnp.float32)
    for number in range(3):
        wrapped = jnp.bitwise_and(numerators[:, number][:, None] * position[None, :], (1 << 20) - 1)
        phase = wrapped.astype(jnp.float32) * (2.0 * math.pi / (1 << 20))
        tone_real = tone_real + levels[:, number][:, None] * jnp.cos(phase)
        tone_imag = tone_imag + levels[:, number][:, None] * jnp.sin(phase)
    result = jnp.stack([noise[:, 0] * envelope + tone_real, noise[:, 1] * envelope + tone_imag], axis=1)
    return result.astype(jnp.bfloat16)


def bell_draw(rng, shape, scale, bound, held_as=jnp.bfloat16):
    array = jax.random.normal(rng, shape, jnp.float32) * scale
    return jnp.minimum(jnp.maximum(array, -bound), bound).astype(held_as)


def setup_inputs(seed: int = 0, part: int = 0) -> dict:
    key_of = jax.random.split(jax.random.key(seed), 3)
    part_keys = jax.random.split(jax.random.fold_in(key_of[2], part), 3)
    signal = draw_signal(jax.random.fold_in(jax.random.fold_in(key_of[2], part), 71), part)
    taps = bell_draw(key_of[1], (TAPS, CHANNELS), TAPS ** -0.5, 1.5, jnp.float32)
    return {"signal": signal, "taps": taps}


def reference(signal, taps):
    streams = signal.shape[0]
    frames = signal.astype(jnp.float32).reshape(streams, 2, FRAMES, CHANNELS)
    padded = jnp.pad(frames, ((0, 0), (0, 0), (TAPS - 1, 0), (0, 0)))
    filtered = jnp.zeros((streams, 2, FRAMES, CHANNELS), jnp.float32)
    for tap_index in range(TAPS):
        start = TAPS - 1 - tap_index
        filtered = filtered + taps[tap_index] * padded[:, :, start:start + FRAMES, :]
    spectrum = jnp.fft.fft(lax.complex(filtered[:, 0], filtered[:, 1]), axis=-1) / RADIX
    real_part = jnp.real(spectrum)
    imag_part = jnp.imag(spectrum)
    power = lax.optimization_barrier(jnp.mean(real_part * real_part + imag_part * imag_part, axis=1))
    factor = 1.0 / jnp.sqrt(power + 1.0)
    stacked = jnp.stack([real_part * factor[:, None, :], imag_part * factor[:, None, :]], axis=1)
    return jnp.transpose(stacked, (0, 1, 3, 2))
```

```python
import math

import jax
import jax.numpy as jnp
import numpy as np
from jax import lax
from jax.experimental import pallas as pl
from jax.experimental.pallas import tpu as pltpu
from jax.sharding import PartitionSpec as P


SLOW = 32
LANES = 128
TURN = 16
POWER = 12
FLOOR = 2.0**-10.25
REACH = 2.0**10.25


def tables(channels):
    slow = np.arange(SLOW)[:, None]
    fast = np.arange(LANES)[None, :]
    angle = -2.0 * math.pi * slow * fast / channels
    twist = np.stack([np.cos(angle), np.sin(angle)]).astype(np.float32)
    turn = 2.0 * math.pi * (np.arange(LANES)[:, None] * fast % LANES) / LANES
    cosine, sine = np.cos(turn), np.sin(turn)
    matrix = np.block([[cosine, sine], [-sine, cosine]]) / math.sqrt(channels)
    high = matrix.astype(jnp.bfloat16)
    low = (matrix - high.astype(np.float64)).astype(jnp.bfloat16)
    return twist, high, low


def turned(value, numerator, denominator):
    real, imag = value
    eighth = (8 * numerator) % (8 * denominator)
    if eighth % denominator == 0:
        step = eighth // denominator
        half = math.sqrt(0.5)
        return [
            lambda: (real, imag),
            lambda: ((real + imag) * half, (imag - real) * half),
            lambda: (imag, -real),
            lambda: ((imag - real) * half, (real + imag) * -half),
            lambda: (-real, -imag),
            lambda: ((real + imag) * -half, (real - imag) * half),
            lambda: (-imag, real),
            lambda: ((real - imag) * half, (real + imag) * half),
        ][step]()
    angle = -2.0 * math.pi * numerator / denominator
    cosine, sine = math.cos(angle), math.sin(angle)
    return (real * cosine - imag * sine, real * sine + imag * cosine)


def fourier(values):
    count = len(values)
    if count == 1:
        return values
    even = fourier(values[0::2])
    odd = fourier(values[1::2])
    odd = [turned(item, index, count) for index, item in enumerate(odd)]
    upper = [(a[0] + b[0], a[1] + b[1]) for a, b in zip(even, odd)]
    lower = [(a[0] - b[0], a[1] - b[1]) for a, b in zip(even, odd)]
    return upper + lower


def encode_kernel(place, frames, edge, taps, twist, high, low, *rest):
    pieces = rest[:8]
    window, grid, split_high, split_low, rows = rest[8:]
    depth = taps.shape[0]
    count = frames.shape[1]
    lead = edge.shape[1]
    me = place[0]

    def filter_step(step, largest):
        part = step // SLOW
        slow = step % SLOW
        columns = pl.ds(pl.multiple_of(slow * LANES, LANES), LANES)
        window[pl.ds(0, lead), :] = edge[part, :, columns].astype(jnp.float32)
        window[pl.ds(lead, count), :] = frames[part, :, columns].astype(jnp.float32)
        weights = [taps[pl.ds(k, 1), columns] for k in range(depth)]
        for block in range(count // 8):
            total = None
            for k in range(depth):
                term = weights[k] * window[pl.ds(lead + block * 8 - k, 8), :]
                total = term if total is None else total + term
            grid[part, slow, pl.ds(block * 8, 8), :] = total
            largest = jnp.maximum(largest, jnp.abs(total))
        return largest

    largest = lax.fori_loop(0, 2 * SLOW, filter_step, jnp.zeros((8, LANES), jnp.float32))
    bound = jnp.max(largest) * (math.sqrt(2.0 * LANES * SLOW))
    scale = jnp.full((8, LANES), REACH, jnp.float32) / jnp.maximum(bound, 1e-35)
    scale = scale.astype(jnp.bfloat16).astype(jnp.float32)

    def slow_step(block, carry):
        times = pl.ds(pl.multiple_of(block * TURN, TURN), TURN)
        for j in range(4):
            column = [(grid[0, 4 * i + j, times, :], grid[1, 4 * i + j, times, :]) for i in range(8)]
            for u, item in enumerate(fourier(column)):
                real, imag = turned(item, j * u, SLOW)
                grid[0, 4 * u + j, times, :] = real
                grid[1, 4 * u + j, times, :] = imag
        for u in range(8):
            column = [(grid[0, 4 * u + j, times, :], grid[1, 4 * u + j, times, :]) for j in range(4)]
            for w, (real, imag) in enumerate(fourier(column)):
                slow = u + 8 * w
                cosine = twist[0, pl.ds(slow, 1), :]
                sine = twist[1, pl.ds(slow, 1), :]
                for part, value in enumerate((real * cosine - imag * sine, real * sine + imag * cosine)):
                    top = value.astype(jnp.bfloat16)
                    lanes = pl.ds(part * LANES, LANES)
                    split_high[slow, times, lanes] = top
                    split_low[slow, times, lanes] = (value - top.astype(jnp.float32)).astype(jnp.bfloat16)
        return carry

    lax.fori_loop(0, count // TURN, slow_step, 0)

    def product(left, right):
        return lax.dot_general(left, right, (((1,), (1,)), ((), ())), preferred_element_type=jnp.float32)

    def fast_step(slow, carry):
        near = split_high[slow]
        value = product(high[...], near) + product(low[...], near) + product(high[...], split_low[slow])
        for part in range(2):
            rows[part, pl.ds(slow, LANES, stride=SLOW), :] = value[part * LANES : (part + 1) * LANES]
        return carry

    lax.fori_loop(0, SLOW, fast_step, 0)

    width = LANES * SLOW // 8
    for d in range(8):
        first = jnp.bitwise_xor(me, d) * width
        for part in range(2):

            def code_step(step, carry):
                start = pl.multiple_of(first + step * 64, 64)
                value = rows[part, pl.ds(start, 64), :]
                level = jnp.abs(value) * scale[:1] + FLOOR
                square = level * level
                sixth = square * level
                sixth = sixth * sixth
                level = sixth * sixth
                level = jnp.where(value < 0.0, -level, level)
                pieces[d][pl.ds(pl.multiple_of(part * width + step * 64, 64), 64), :] = level.astype(jnp.bfloat16)
                return carry

            lax.fori_loop(0, width // 64, code_step, 0)
        pieces[d][pl.ds(2 * width, 16), :] = jnp.concatenate([scale, scale], axis=0).astype(jnp.bfloat16)


def encode(place, frames, edge, taps, twist, high, low):
    count, channels = frames.shape[1:]
    piece = jax.ShapeDtypeStruct((2 * channels // 8 + 16, count), jnp.bfloat16)
    whole = pl.BlockSpec(memory_space=pltpu.VMEM)
    return pl.pallas_call(
        encode_kernel,
        out_shape=[piece] * 8,
        in_specs=[pl.BlockSpec(memory_space=pltpu.SMEM)] + [whole] * 6,
        out_specs=[whole] * 8,
        scratch_shapes=[
            pltpu.VMEM((16 + count, LANES), jnp.float32),
            pltpu.VMEM((2, SLOW, count, LANES), jnp.float32),
            pltpu.VMEM((SLOW, count, 2 * LANES), jnp.bfloat16),
            pltpu.VMEM((SLOW, count, 2 * LANES), jnp.bfloat16),
            pltpu.VMEM((2, channels, LANES), jnp.float32),
        ],
        compiler_params=pltpu.CompilerParams(vmem_limit_bytes=48 * 1024 * 1024),
        name="encode",
    )(place, frames, edge, taps, twist, high, low)


def decode_kernel(place, *rest):
    pieces = rest[:8]
    output = rest[-1]
    width = output.shape[2]
    half = (pieces[0].shape[0] - 16) // 2
    me = place[0]
    base = pl.program_id(0) * width
    inverse = [1.0 / pieces[d][pl.ds(2 * half, 16), :].astype(jnp.float32) for d in range(8)]

    def step(number, carry):
        power = None
        found = []
        for d in range(8):
            for part in range(2):
                start = pl.multiple_of(part * half + base + number * 16, 16)
                code = pieces[d][pl.ds(start, 16), :].astype(jnp.float32)
                level = jnp.exp2(jnp.log2(jnp.abs(code)) * (1.0 / POWER)) - FLOOR
                level = level * inverse[d]
                found.append(jnp.where(code < 0.0, -level, level))
                power = level * level if power is None else power + level * level
        total = jnp.sum(power, axis=1, keepdims=True)
        factor = lax.rsqrt(total / (8 * LANES) + 1.0)
        for d in range(8):
            lanes = pl.ds(pl.multiple_of(jnp.bitwise_xor(me, d) * LANES, LANES), LANES)
            for part in range(2):
                output[0, part, pl.ds(pl.multiple_of(number * 16, 16), 16), lanes] = found[2 * d + part] * factor
        return carry

    lax.fori_loop(0, width // 16, step, 0)


def decode(place, pieces, stream, streams, before):
    half = (pieces[0].shape[0] - 16) // 2
    blocks = 8
    shape = (streams, 2, half, 8 * LANES)
    whole = pl.BlockSpec(memory_space=pltpu.VMEM)
    operands = [place, *pieces]
    in_specs = [pl.BlockSpec(memory_space=pltpu.SMEM)] + [whole] * 8
    aliases = {}
    if before is not None:
        operands.append(before)
        in_specs.append(pl.BlockSpec(memory_space=pl.ANY))
        aliases = {9: 0}
    return pl.pallas_call(
        decode_kernel,
        grid=(blocks,),
        out_shape=jax.ShapeDtypeStruct(shape, jnp.float32),
        in_specs=in_specs,
        out_specs=pl.BlockSpec((1, 2, half // blocks, 8 * LANES), lambda i: (stream, 0, i, 0)),
        input_output_aliases=aliases,
        compiler_params=pltpu.CompilerParams(vmem_limit_bytes=48 * 1024 * 1024),
        name="decode",
    )(*operands)


def shards(signal, taps):
    streams = signal.shape[0]
    channels = taps.shape[1]
    count = signal.shape[2] // channels
    size = lax.axis_size("tm")
    place = lax.axis_index("tm").astype(jnp.int32)[None]
    twist, high, low = tables(channels)
    frames = signal.reshape(streams, 2, count, channels)
    route = [(i, i + 1) for i in range(size - 1)]
    sent = []
    for stream in range(streams):
        edge = lax.ppermute(frames[stream, :, count - 16 :, :], "tm", route)
        sent.append(encode(place, frames[stream], edge, taps, twist, high, low))
    output = None
    for stream in range(streams):
        pieces = [sent[stream][0]]
        for d in range(1, size):
            pieces.append(lax.ppermute(sent[stream][d], "tm", [(i, i ^ d) for i in range(size)]))
        output = decode(place, pieces, stream, streams, output)
    return output


def solution(mesh):
    in_specs = (P("stream", None, "tm"), P())
    out_specs = P("stream", None, "tm", None)
    return jax.shard_map(shards, mesh=mesh, in_specs=in_specs, out_specs=out_specs, check_vma=False)
```

```python
import math

import jax
import jax.numpy as jnp
import numpy as np
from jax import lax
from jax.experimental import pallas as pl
from jax.experimental.pallas import tpu as pltpu
from jax.sharding import PartitionSpec as P


SLOW = 32
LANES = 128
TURN = 16
LEAD = 16
PAIR = 2
UNROLL = 4
PITCH = 36
POWER = 12
FLOOR = 2.0**-10.25
REACH = 2.0**10.25


def tables(channels):
    slow = np.arange(SLOW)[:, None]
    fast = np.arange(LANES)[None, :]
    angle = -2.0 * math.pi * slow * fast / channels
    twist = np.stack([np.cos(angle), np.sin(angle)]).astype(np.float32)
    turn = 2.0 * math.pi * (np.arange(LANES)[:, None] * fast % LANES) / LANES
    cosine, sine = np.cos(turn), np.sin(turn)
    matrix = np.block([[cosine, sine], [-sine, cosine]]) / math.sqrt(channels)
    high = matrix.astype(jnp.bfloat16)
    low = (matrix - high.astype(np.float64)).astype(jnp.bfloat16)
    return twist, np.concatenate([high, low, high], axis=1)


def turned(value, numerator, denominator):
    real, imag = value
    eighth = (8 * numerator) % (8 * denominator)
    if eighth % denominator == 0:
        step = eighth // denominator
        half = math.sqrt(0.5)
        return [
            lambda: (real, imag),
            lambda: ((real + imag) * half, (imag - real) * half),
            lambda: (imag, -real),
            lambda: ((imag - real) * half, (real + imag) * -half),
            lambda: (-real, -imag),
            lambda: ((real + imag) * -half, (real - imag) * half),
            lambda: (-imag, real),
            lambda: ((real - imag) * half, (real + imag) * half),
        ][step]()
    angle = -2.0 * math.pi * numerator / denominator
    cosine, sine = math.cos(angle), math.sin(angle)
    return (real * cosine - imag * sine, real * sine + imag * cosine)


def fourier(values):
    count = len(values)
    if count == 1:
        return values
    even = fourier(values[0::2])
    odd = fourier(values[1::2])
    odd = [turned(item, index, count) for index, item in enumerate(odd)]
    upper = [(a[0] + b[0], a[1] + b[1]) for a, b in zip(even, odd)]
    lower = [(a[0] - b[0], a[1] - b[1]) for a, b in zip(even, odd)]
    return upper + lower


def filter_kernel(frames, taps, grid, largest, window):
    depth = taps.shape[0]
    count = frames.shape[1]
    window[pl.ds(0, LEAD), :] = jnp.zeros((LEAD, LANES), jnp.float32)

    def step(number, most):
        part = number // SLOW
        slow = number % SLOW
        columns = pl.ds(pl.multiple_of(slow * LANES, LANES), LANES)
        window[pl.ds(LEAD, count), :] = frames[part, :, columns].astype(jnp.float32)
        weights = [taps[pl.ds(k, 1), columns] for k in range(depth)]
        for block in range(count // 8):
            total = None
            for k in range(depth):
                if 8 * block + 7 < k:
                    continue
                term = weights[k] * window[pl.ds(LEAD + block * 8 - k, 8), :]
                total = term if total is None else total + term
            grid[part, slow, pl.ds(block * 8, 8), :] = total
            most = jnp.maximum(most, jnp.abs(total))
        return most

    largest[...] = lax.fori_loop(0, 2 * SLOW, step, jnp.zeros((8, LANES), jnp.float32))


def filtered(frames, taps):
    count = frames.shape[1]
    whole = pl.BlockSpec(memory_space=pltpu.VMEM)
    return pl.pallas_call(
        filter_kernel,
        out_shape=[
            jax.ShapeDtypeStruct((2, SLOW, count, LANES), jnp.float32),
            jax.ShapeDtypeStruct((8, LANES), jnp.float32),
        ],
        in_specs=[whole] * 2,
        out_specs=[whole] * 2,
        scratch_shapes=[pltpu.VMEM((LEAD + count, LANES), jnp.float32)],
        compiler_params=pltpu.CompilerParams(vmem_limit_bytes=12 * 1024 * 1024),
        name="filter",
    )(frames, taps)


def encode_kernel(place, edge, taps, grid, largest, twist, matrix, *rest):
    pieces = rest[:8]
    window, head, half, split_high, split_low, rows = rest[8:]
    depth = taps.shape[0]
    count = grid.shape[2]
    me = place[0]
    window[pl.ds(LEAD, LEAD), :] = jnp.zeros((LEAD, LANES), jnp.float32)

    def head_step(number, most):
        part = number // SLOW
        slow = number % SLOW
        columns = pl.ds(pl.multiple_of(slow * LANES, LANES), LANES)
        window[pl.ds(0, LEAD), :] = edge[part, :, columns].astype(jnp.float32)
        weights = [taps[pl.ds(k, 1), columns] for k in range(depth)]
        for block in range(LEAD // 8):
            times = pl.ds(block * 8, 8)
            total = grid[part, slow, times, :]
            for k in range(8 * block + 1, depth):
                total = total + weights[k] * window[pl.ds(LEAD + block * 8 - k, 8), :]
            head[part, slow, times, :] = total
            most = jnp.maximum(most, jnp.abs(total))
        return most

    most = lax.fori_loop(0, 2 * SLOW, head_step, largest[...], unroll=4)
    bound = jnp.max(most) * math.sqrt(2.0 * LANES * SLOW)
    scale = jnp.full((8, LANES), REACH, jnp.float32) / jnp.maximum(bound, 1e-35)
    scale = scale.astype(jnp.bfloat16).astype(jnp.float32)

    def slow_block(source, times):
        for j in range(4):
            column = [(source[0, 4 * i + j, times, :], source[1, 4 * i + j, times, :]) for i in range(8)]
            for u, item in enumerate(fourier(column)):
                real, imag = turned(item, j * u, SLOW)
                half[0, 4 * u + j] = real
                half[1, 4 * u + j] = imag
        for u in range(8):
            column = [(half[0, 4 * u + j], half[1, 4 * u + j]) for j in range(4)]
            for w, (real, imag) in enumerate(fourier(column)):
                slow = u + 8 * w
                cosine = twist[0, pl.ds(slow, 1), :]
                sine = twist[1, pl.ds(slow, 1), :]
                for part, value in enumerate((real * cosine - imag * sine, real * sine + imag * cosine)):
                    top = value.astype(jnp.bfloat16)
                    lanes = pl.ds(part * LANES, LANES)
                    split_high[slow, times, lanes] = top
                    split_low[slow, times, lanes] = (value - top.astype(jnp.float32)).astype(jnp.bfloat16)

    def slow_step(block, carry):
        slow_block(grid, pl.ds(pl.multiple_of(block * TURN, TURN), TURN))
        return carry

    slow_block(head, pl.ds(0, TURN))
    lax.fori_loop(1, count // TURN, slow_step, 0)

    def fast_step(number, carry):
        near = split_high[pl.ds(number * PAIR, PAIR)].reshape(PAIR * count, 2 * LANES)
        far = split_low[pl.ds(number * PAIR, PAIR)].reshape(PAIR * count, 2 * LANES)
        both = jnp.concatenate([near, near, far], axis=1)
        value = lax.dot_general(
            matrix[...], both, (((1,), (1,)), ((), ())), preferred_element_type=jnp.float32
        )
        level = jnp.abs(value) * scale[:1, :1] + FLOOR
        square = level * level
        sixth = square * level
        sixth = sixth * sixth
        level = sixth * sixth
        level = jnp.where(value < 0.0, -level, level)
        for part in range(2):
            for item in range(PAIR):
                rows[part, pl.ds(number * PAIR + item, LANES, stride=PITCH), :] = level[
                    part * LANES : (part + 1) * LANES, item * count : (item + 1) * count
                ]
        return carry

    lax.fori_loop(0, SLOW // PAIR, fast_step, 0, unroll=UNROLL)

    share = LANES // 8
    for d in range(8):
        first = jnp.bitwise_xor(me, d) * share * PITCH
        for part in range(2):
            for fast in range(share):
                start = pl.multiple_of(first + fast * PITCH, 4)
                pieces[d][pl.ds((part * share + fast) * SLOW, SLOW), :] = rows[
                    part, pl.ds(start, SLOW), :
                ].astype(jnp.bfloat16)
        pieces[d][pl.ds(2 * share * SLOW, 16), :] = jnp.concatenate([scale, scale], axis=0).astype(jnp.bfloat16)


def encode(place, edge, taps, grid, largest, twist, matrix):
    count = grid.shape[2]
    channels = taps.shape[1]
    piece = jax.ShapeDtypeStruct((2 * channels // 8 + 16, count), jnp.bfloat16)
    whole = pl.BlockSpec(memory_space=pltpu.VMEM)
    return pl.pallas_call(
        encode_kernel,
        out_shape=[piece] * 8,
        in_specs=[pl.BlockSpec(memory_space=pltpu.SMEM)] + [whole] * 6,
        out_specs=[whole] * 8,
        scratch_shapes=[
            pltpu.VMEM((2 * LEAD, LANES), jnp.float32),
            pltpu.VMEM((2, SLOW, LEAD, LANES), jnp.float32),
            pltpu.VMEM((2, SLOW, TURN, LANES), jnp.float32),
            pltpu.VMEM((SLOW, count, 2 * LANES), jnp.bfloat16),
            pltpu.VMEM((SLOW, count, 2 * LANES), jnp.bfloat16),
            pltpu.VMEM((2, PITCH * LANES, LANES), jnp.float32),
        ],
        compiler_params=pltpu.CompilerParams(vmem_limit_bytes=20 * 1024 * 1024),
        name="encode",
    )(place, edge, taps, grid, largest, twist, matrix)


def decode_kernel(place, *rest):
    pieces = rest[:8]
    output = rest[-1]
    width = output.shape[2]
    half = (pieces[0].shape[0] - 16) // 2
    me = place[0]
    base = pl.program_id(0) * width
    inverse = [1.0 / pieces[d][pl.ds(2 * half, 16), :].astype(jnp.float32) for d in range(8)]

    def step(number, carry):
        power = None
        found = []
        for d in range(8):
            for part in range(2):
                start = pl.multiple_of(part * half + base + number * 16, 16)
                code = pieces[d][pl.ds(start, 16), :].astype(jnp.float32)
                level = jnp.exp2(jnp.log2(jnp.abs(code)) * (1.0 / POWER)) - FLOOR
                level = level * inverse[d]
                found.append(jnp.where(code < 0.0, -level, level))
                power = level * level if power is None else power + level * level
        total = jnp.sum(power, axis=1, keepdims=True)
        factor = lax.rsqrt(total / (8 * LANES) + 1.0)
        for d in range(8):
            lanes = pl.ds(pl.multiple_of(jnp.bitwise_xor(me, d) * LANES, LANES), LANES)
            for part in range(2):
                output[0, part, pl.ds(pl.multiple_of(number * 16, 16), 16), lanes] = found[2 * d + part] * factor
        return carry

    lax.fori_loop(0, width // 16, step, 0, unroll=4)


def decode(place, pieces, stream, streams, before):
    half = (pieces[0].shape[0] - 16) // 2
    blocks = 4
    shape = (streams, 2, half, 8 * LANES)
    whole = pl.BlockSpec(memory_space=pltpu.VMEM)
    operands = [place, *pieces]
    in_specs = [pl.BlockSpec(memory_space=pltpu.SMEM)] + [whole] * 8
    aliases = {}
    if before is not None:
        operands.append(before)
        in_specs.append(pl.BlockSpec(memory_space=pl.ANY))
        aliases = {9: 0}
    return pl.pallas_call(
        decode_kernel,
        grid=(blocks,),
        out_shape=jax.ShapeDtypeStruct(shape, jnp.float32),
        in_specs=in_specs,
        out_specs=pl.BlockSpec((1, 2, half // blocks, 8 * LANES), lambda i: (stream, 0, i, 0)),
        input_output_aliases=aliases,
        compiler_params=pltpu.CompilerParams(vmem_limit_bytes=16 * 1024 * 1024),
        name="decode",
    )(*operands)


def shards(signal, taps):
    streams = signal.shape[0]
    channels = taps.shape[1]
    count = signal.shape[2] // channels
    size = lax.axis_size("tm")
    place = lax.axis_index("tm").astype(jnp.int32)[None]
    twist, matrix = tables(channels)
    route = [(i, i + 1) for i in range(size - 1)]
    tail = signal[:, :, (count - LEAD) * channels :]
    edges = [lax.ppermute(tail[stream], "tm", route) for stream in range(streams)]
    arrived = []
    held = signal
    for stream in range(streams):
        frames = held[stream].reshape(2, count, channels)
        grid, largest = filtered(frames, taps)
        edge = edges[stream].reshape(2, LEAD, channels)
        pieces = list(encode(place, edge, taps, grid, largest, twist, matrix))
        held, pieces[0] = lax.optimization_barrier((held, pieces[0]))
        for d in range(1, size):
            pieces[d] = lax.ppermute(pieces[d], "tm", [(i, i ^ d) for i in range(size)])
        arrived.append(pieces)
    output = None
    for stream in range(streams):
        output = decode(place, arrived[stream], stream, streams, output)
    return output


def solution(mesh):
    in_specs = (P("stream", None, "tm"), P())
    out_specs = P("stream", None, "tm", None)
    return jax.shard_map(shards, mesh=mesh, in_specs=in_specs, out_specs=out_specs, check_vma=False)
```

```python
import itertools
import math

import jax
import jax.numpy as jnp
import numpy as np
from jax import lax
from jax.experimental import pallas as pl
from jax.experimental.pallas import tpu as pltpu
from jax.sharding import PartitionSpec as P


SLOW = 32
LANES = 128
TURN = 16
LEAD = 16
PAIR = 4
UNROLL = 4
PITCH = 36
ORDER = (5, 1, 4, 7, 2, 3, 6)
POWER = 12
FLOOR = 2.0**-10.25
REACH = 2.0**10.25


def tables(channels):
    slow = np.arange(SLOW)[:, None]
    fast = np.arange(LANES)[None, :]
    angle = -2.0 * math.pi * slow * fast / channels
    twist = np.stack([np.cos(angle), np.sin(angle)]).astype(np.float32)
    turn = 2.0 * math.pi * (np.arange(LANES)[:, None] * fast % LANES) / LANES
    cosine, sine = np.cos(turn), np.sin(turn)
    matrix = np.block([[cosine, sine], [-sine, cosine]]) / math.sqrt(channels)
    high = matrix.astype(jnp.bfloat16)
    low = (matrix - high.astype(np.float64)).astype(jnp.bfloat16)
    return twist, np.concatenate([high, low, high], axis=1)


def turned(value, numerator, denominator):
    real, imag = value
    eighth = (8 * numerator) % (8 * denominator)
    if eighth % denominator == 0:
        step = eighth // denominator
        half = math.sqrt(0.5)
        return [
            lambda: (real, imag),
            lambda: ((real + imag) * half, (imag - real) * half),
            lambda: (imag, -real),
            lambda: ((imag - real) * half, (real + imag) * -half),
            lambda: (-real, -imag),
            lambda: ((real + imag) * -half, (real - imag) * half),
            lambda: (-imag, real),
            lambda: ((real - imag) * half, (real + imag) * half),
        ][step]()
    angle = -2.0 * math.pi * numerator / denominator
    cosine, sine = math.cos(angle), math.sin(angle)
    return (real * cosine - imag * sine, real * sine + imag * cosine)


def fourier(values):
    count = len(values)
    if count == 1:
        return values
    even = fourier(values[0::2])
    odd = fourier(values[1::2])
    odd = [turned(item, index, count) for index, item in enumerate(odd)]
    upper = [(a[0] + b[0], a[1] + b[1]) for a, b in zip(even, odd)]
    lower = [(a[0] - b[0], a[1] - b[1]) for a, b in zip(even, odd)]
    return upper + lower


def filter_kernel(frames, taps, grid, largest, window):
    depth = taps.shape[0]
    count = frames.shape[1]
    window[:, pl.ds(0, LEAD), :] = jnp.zeros((2, LEAD, LANES), jnp.float32)

    def step(slow, most):
        columns = pl.ds(pl.multiple_of(slow * LANES, LANES), LANES)
        weights = [taps[pl.ds(k, 1), columns] for k in range(depth)]
        for part in range(2):
            window[part, pl.ds(LEAD, count), :] = frames[part, :, columns].astype(jnp.float32)
        for part, block in itertools.product(range(2), range(count // 8)):
            total = None
            for k in range(depth):
                if 8 * block + 7 < k:
                    continue
                term = weights[k] * window[part, pl.ds(LEAD + block * 8 - k, 8), :]
                total = term if total is None else total + term
            grid[part, slow, pl.ds(block * 8, 8), :] = total
            most = jnp.maximum(most, jnp.abs(total))
        return most

    largest[...] = lax.fori_loop(0, SLOW, step, jnp.zeros((8, LANES), jnp.float32), unroll=2)


def filtered(frames, taps):
    count = frames.shape[1]
    whole = pl.BlockSpec(memory_space=pltpu.VMEM)
    return pl.pallas_call(
        filter_kernel,
        out_shape=[
            jax.ShapeDtypeStruct((2, SLOW, count, LANES), jnp.float32),
            jax.ShapeDtypeStruct((8, LANES), jnp.float32),
        ],
        in_specs=[whole] * 2,
        out_specs=[whole] * 2,
        scratch_shapes=[pltpu.VMEM((2, LEAD + count, LANES), jnp.float32)],
        compiler_params=pltpu.CompilerParams(vmem_limit_bytes=12 * 1024 * 1024),
        name="filter",
    )(frames, taps)


def encode_kernel(edge, taps, grid, largest, twist, matrix, *rest):
    pieces = rest[:8]
    window, head, half, split_high, split_low, rows = rest[8:]
    depth = taps.shape[0]
    count = grid.shape[2]
    me = lax.axis_index("tm")
    window[pl.ds(LEAD, LEAD), :] = jnp.zeros((LEAD, LANES), jnp.float32)

    def head_step(number, most):
        part = number // SLOW
        slow = number % SLOW
        columns = pl.ds(pl.multiple_of(slow * LANES, LANES), LANES)
        window[pl.ds(0, LEAD), :] = edge[part, :, columns].astype(jnp.float32)
        weights = [taps[pl.ds(k, 1), columns] for k in range(depth)]
        for block in range(LEAD // 8):
            times = pl.ds(block * 8, 8)
            total = grid[part, slow, times, :]
            for k in range(8 * block + 1, depth):
                total = total + weights[k] * window[pl.ds(LEAD + block * 8 - k, 8), :]
            head[part, slow, times, :] = total
            most = jnp.maximum(most, jnp.abs(total))
        return most

    most = lax.fori_loop(0, 2 * SLOW, head_step, largest[...], unroll=4)
    bound = jnp.max(most) * math.sqrt(2.0 * LANES * SLOW)
    scale = jnp.full((8, LANES), REACH, jnp.float32) / jnp.maximum(bound, 1e-35)
    scale = scale.astype(jnp.bfloat16).astype(jnp.float32)

    def slow_block(source, times):
        for j in range(4):
            column = [(source[0, 4 * i + j, times, :], source[1, 4 * i + j, times, :]) for i in range(8)]
            for u, item in enumerate(fourier(column)):
                real, imag = turned(item, j * u, SLOW)
                half[0, 4 * u + j] = real
                half[1, 4 * u + j] = imag
        for u in range(8):
            column = [(half[0, 4 * u + j], half[1, 4 * u + j]) for j in range(4)]
            for w, (real, imag) in enumerate(fourier(column)):
                slow = u + 8 * w
                cosine = twist[0, pl.ds(slow, 1), :]
                sine = twist[1, pl.ds(slow, 1), :]
                for part, value in enumerate((real * cosine - imag * sine, real * sine + imag * cosine)):
                    top = value.astype(jnp.bfloat16)
                    lanes = pl.ds(part * LANES, LANES)
                    split_high[slow, times, lanes] = top
                    split_low[slow, times, lanes] = (value - top.astype(jnp.float32)).astype(jnp.bfloat16)

    def slow_step(block, carry):
        slow_block(grid, pl.ds(pl.multiple_of(block * TURN, TURN), TURN))
        return carry

    slow_block(head, pl.ds(0, TURN))
    lax.fori_loop(1, count // TURN, slow_step, 0)

    def fast_step(number, carry):
        near = split_high[pl.ds(number * PAIR, PAIR)].reshape(PAIR * count, 2 * LANES)
        far = split_low[pl.ds(number * PAIR, PAIR)].reshape(PAIR * count, 2 * LANES)
        both = jnp.concatenate([near, near, far], axis=1)
        value = lax.dot_general(
            matrix[...], both, (((1,), (1,)), ((), ())), preferred_element_type=jnp.float32
        )
        level = jnp.abs(value) * scale[:1, :1] + FLOOR
        square = level * level
        sixth = square * level
        sixth = sixth * sixth
        level = sixth * sixth
        level = jnp.where(value < 0.0, -level, level)
        for part in range(2):
            for item in range(PAIR):
                rows[part, pl.ds(number * PAIR + item, LANES, stride=PITCH), :] = level[
                    part * LANES : (part + 1) * LANES, item * count : (item + 1) * count
                ]
        return carry

    lax.fori_loop(0, SLOW // PAIR, fast_step, 0, unroll=UNROLL)

    share = LANES // 8
    for d in range(8):
        first = jnp.bitwise_xor(me, d) * share * PITCH
        for part in range(2):
            for fast in range(share):
                start = pl.multiple_of(first + fast * PITCH, 4)
                pieces[d][pl.ds((part * share + fast) * SLOW, SLOW), :] = rows[
                    part, pl.ds(start, SLOW), :
                ].astype(jnp.bfloat16)
        pieces[d][pl.ds(2 * share * SLOW, 16), :] = jnp.concatenate([scale, scale], axis=0).astype(jnp.bfloat16)


def encode(edge, taps, grid, largest, twist, matrix):
    count = grid.shape[2]
    channels = taps.shape[1]
    piece = jax.ShapeDtypeStruct((2 * channels // 8 + 16, count), jnp.bfloat16)
    whole = pl.BlockSpec(memory_space=pltpu.VMEM)
    return pl.pallas_call(
        encode_kernel,
        out_shape=[piece] * 8,
        in_specs=[whole] * 6,
        out_specs=[whole] * 8,
        scratch_shapes=[
            pltpu.VMEM((2 * LEAD, LANES), jnp.float32),
            pltpu.VMEM((2, SLOW, LEAD, LANES), jnp.float32),
            pltpu.VMEM((2, SLOW, TURN, LANES), jnp.float32),
            pltpu.VMEM((SLOW, count, 2 * LANES), jnp.bfloat16),
            pltpu.VMEM((SLOW, count, 2 * LANES), jnp.bfloat16),
            pltpu.VMEM((2, PITCH * LANES, LANES), jnp.float32),
        ],
        compiler_params=pltpu.CompilerParams(vmem_limit_bytes=20 * 1024 * 1024),
        name="encode",
    )(edge, taps, grid, largest, twist, matrix)


def decode_kernel(*rest):
    pieces = rest[:8]
    output = rest[-1]
    width = output.shape[2]
    half = (pieces[0].shape[0] - 16) // 2
    me = lax.axis_index("tm")
    base = pl.program_id(0) * width
    inverse = [1.0 / pieces[d][pl.ds(2 * half, 16), :].astype(jnp.float32) for d in range(8)]

    def step(number, carry):
        power = None
        found = []
        for d in range(8):
            for part in range(2):
                start = pl.multiple_of(part * half + base + number * 16, 16)
                code = pieces[d][pl.ds(start, 16), :].astype(jnp.float32)
                level = jnp.exp2(jnp.log2(jnp.abs(code)) * (1.0 / POWER)) - FLOOR
                level = level * inverse[d]
                found.append(jnp.where(code < 0.0, -level, level))
                power = level * level if power is None else power + level * level
        total = jnp.sum(power, axis=1, keepdims=True)
        factor = lax.rsqrt(total / (8 * LANES) + 1.0)
        for d in range(8):
            lanes = pl.ds(pl.multiple_of(jnp.bitwise_xor(me, d) * LANES, LANES), LANES)
            for part in range(2):
                output[0, part, pl.ds(pl.multiple_of(number * 16, 16), 16), lanes] = found[2 * d + part] * factor
        return carry

    lax.fori_loop(0, width // 16, step, 0, unroll=4)


def decode(pieces, stream, streams, before):
    half = (pieces[0].shape[0] - 16) // 2
    blocks = 4
    shape = (streams, 2, half, 8 * LANES)
    whole = pl.BlockSpec(memory_space=pltpu.VMEM)
    operands = [*pieces]
    in_specs = [whole] * 8
    aliases = {}
    if before is not None:
        operands.append(before)
        in_specs.append(pl.BlockSpec(memory_space=pl.ANY))
        aliases = {8: 0}
    return pl.pallas_call(
        decode_kernel,
        grid=(blocks,),
        out_shape=jax.ShapeDtypeStruct(shape, jnp.float32),
        in_specs=in_specs,
        out_specs=pl.BlockSpec((1, 2, half // blocks, 8 * LANES), lambda i: (stream, 0, i, 0)),
        input_output_aliases=aliases,
        compiler_params=pltpu.CompilerParams(vmem_limit_bytes=16 * 1024 * 1024),
        name="decode",
    )(*operands)


def shards(signal, taps):
    streams = signal.shape[0]
    channels = taps.shape[1]
    count = signal.shape[2] // channels
    size = lax.axis_size("tm")
    twist, matrix = tables(channels)
    route = [(i, i + 1) for i in range(size - 1)]
    last = (count - LEAD) * channels
    tail = signal[:1, :, last:]
    edge = lax.ppermute(tail, "tm", route)
    held, tail = lax.optimization_barrier((signal, tail))
    arrived = []
    for stream in range(streams):
        frames = held[stream].reshape(2, count, channels)
        grid, largest = filtered(frames, taps)
        near = edge.reshape(2, LEAD, channels)
        if stream + 1 < streams:
            tail = held[stream + 1 : stream + 2, :, last:]
            tail, largest = lax.optimization_barrier((tail, largest))
            edge = lax.ppermute(tail, "tm", route)
        pieces = list(encode(near, taps, grid, largest, twist, matrix))
        held, pieces[0] = lax.optimization_barrier((held, pieces[0]))
        for d in ORDER:
            pieces[d] = lax.ppermute(pieces[d], "tm", [(i, i ^ d) for i in range(size)])
        arrived.append(pieces)
    output = None
    for stream in range(streams):
        output = decode(arrived[stream], stream, streams, output)
    return output


def solution(mesh):
    in_specs = (P("stream", None, "tm"), P())
    out_specs = P("stream", None, "tm", None)
    return jax.shard_map(shards, mesh=mesh, in_specs=in_specs, out_specs=out_specs, check_vma=False)
```

```python
import itertools
import math

import jax
import jax.numpy as jnp
import numpy as np
from jax import lax
from jax.experimental import pallas as pl
from jax.experimental.pallas import tpu as pltpu
from jax.sharding import PartitionSpec as P


SLOW = 32
LANES = 128
TURN = 16
LEAD = 16
PAIR = 4
UNROLL = 4
PITCH = 36
ORDER = (5, 1, 4, 7, 2, 3, 6)
POWER = 12
FLOOR = 2.0**-10.25
REACH = 2.0**10.25


def tables(channels):
    slow = np.arange(SLOW)[:, None]
    fast = np.arange(LANES)[None, :]
    angle = -2.0 * math.pi * slow * fast / channels
    twist = np.stack([np.cos(angle), np.sin(angle)]).astype(np.float32)
    turn = 2.0 * math.pi * (np.arange(LANES)[:, None] * fast % LANES) / LANES
    cosine, sine = np.cos(turn), np.sin(turn)
    matrix = np.block([[cosine, sine], [-sine, cosine]]) / math.sqrt(channels)
    high = matrix.astype(jnp.bfloat16)
    low = (matrix - high.astype(np.float64)).astype(jnp.bfloat16)
    return twist, np.concatenate([high, low, high], axis=1)


def turned(value, numerator, denominator):
    real, imag = value
    eighth = (8 * numerator) % (8 * denominator)
    if eighth % denominator == 0:
        step = eighth // denominator
        half = math.sqrt(0.5)
        return [
            lambda: (real, imag),
            lambda: ((real + imag) * half, (imag - real) * half),
            lambda: (imag, -real),
            lambda: ((imag - real) * half, (real + imag) * -half),
            lambda: (-real, -imag),
            lambda: ((real + imag) * -half, (real - imag) * half),
            lambda: (-imag, real),
            lambda: ((real - imag) * half, (real + imag) * half),
        ][step]()
    angle = -2.0 * math.pi * numerator / denominator
    cosine, sine = math.cos(angle), math.sin(angle)
    return (real * cosine - imag * sine, real * sine + imag * cosine)


def fourier(values):
    count = len(values)
    if count == 1:
        return values
    even = fourier(values[0::2])
    odd = fourier(values[1::2])
    odd = [turned(item, index, count) for index, item in enumerate(odd)]
    upper = [(a[0] + b[0], a[1] + b[1]) for a, b in zip(even, odd)]
    lower = [(a[0] - b[0], a[1] - b[1]) for a, b in zip(even, odd)]
    return upper + lower


def filter_kernel(frames, taps, grid, largest, window):
    depth = taps.shape[0]
    count = frames.shape[1]
    window[:, pl.ds(0, LEAD), :] = jnp.zeros((2, LEAD, LANES), jnp.float32)

    def step(slow, most):
        columns = pl.ds(pl.multiple_of(slow * LANES, LANES), LANES)
        weights = [taps[pl.ds(k, 1), columns] for k in range(depth)]
        for part in range(2):
            window[part, pl.ds(LEAD, count), :] = frames[part, :, columns].astype(jnp.float32)
        for part, block in itertools.product(range(2), range(count // 8)):
            total = None
            for k in range(depth):
                if 8 * block + 7 < k:
                    continue
                term = weights[k] * window[part, pl.ds(LEAD + block * 8 - k, 8), :]
                total = term if total is None else total + term
            grid[part, slow, pl.ds(block * 8, 8), :] = total
            most = jnp.maximum(most, jnp.abs(total))
        return most

    largest[...] = lax.fori_loop(0, SLOW, step, jnp.zeros((8, LANES), jnp.float32), unroll=2)


def filtered(frames, taps):
    count = frames.shape[1]
    whole = pl.BlockSpec(memory_space=pltpu.VMEM)
    return pl.pallas_call(
        filter_kernel,
        out_shape=[
            jax.ShapeDtypeStruct((2, SLOW, count, LANES), jnp.float32),
            jax.ShapeDtypeStruct((8, LANES), jnp.float32),
        ],
        in_specs=[whole] * 2,
        out_specs=[whole] * 2,
        scratch_shapes=[pltpu.VMEM((2, LEAD + count, LANES), jnp.float32)],
        compiler_params=pltpu.CompilerParams(vmem_limit_bytes=12 * 1024 * 1024),
        name="filter",
    )(frames, taps)


def encode_kernel(edge, taps, grid, largest, twist, matrix, *rest):
    pieces = rest[:8]
    window, head, half, split_high, split_low, rows = rest[8:]
    depth = taps.shape[0]
    count = grid.shape[2]
    me = lax.axis_index("tm")
    window[pl.ds(LEAD, LEAD), :] = jnp.zeros((LEAD, LANES), jnp.float32)

    def head_step(number, most):
        part = number // SLOW
        slow = number % SLOW
        columns = pl.ds(pl.multiple_of(slow * LANES, LANES), LANES)
        window[pl.ds(0, LEAD), :] = edge[part, :, columns].astype(jnp.float32)
        weights = [taps[pl.ds(k, 1), columns] for k in range(depth)]
        for block in range(LEAD // 8):
            times = pl.ds(block * 8, 8)
            total = grid[part, slow, times, :]
            for k in range(8 * block + 1, depth):
                total = total + weights[k] * window[pl.ds(LEAD + block * 8 - k, 8), :]
            head[part, slow, times, :] = total
            most = jnp.maximum(most, jnp.abs(total))
        return most

    most = lax.fori_loop(0, 2 * SLOW, head_step, largest[...], unroll=4)
    bound = jnp.max(most) * math.sqrt(2.0 * LANES * SLOW)
    scale = jnp.full((8, LANES), REACH, jnp.float32) / jnp.maximum(bound, 1e-35)
    scale = scale.astype(jnp.bfloat16).astype(jnp.float32)

    def slow_block(source, times):
        for j in range(4):
            column = [(source[0, 4 * i + j, times, :], source[1, 4 * i + j, times, :]) for i in range(8)]
            for u, item in enumerate(fourier(column)):
                real, imag = turned(item, j * u, SLOW)
                half[0, 4 * u + j] = real
                half[1, 4 * u + j] = imag
        for u in range(8):
            column = [(half[0, 4 * u + j], half[1, 4 * u + j]) for j in range(4)]
            for w, (real, imag) in enumerate(fourier(column)):
                slow = u + 8 * w
                cosine = twist[0, pl.ds(slow, 1), :]
                sine = twist[1, pl.ds(slow, 1), :]
                for part, value in enumerate((real * cosine - imag * sine, real * sine + imag * cosine)):
                    top = value.astype(jnp.bfloat16)
                    lanes = pl.ds(part * LANES, LANES)
                    split_high[slow, times, lanes] = top
                    split_low[slow, times, lanes] = (value - top.astype(jnp.float32)).astype(jnp.bfloat16)

    def slow_step(block, carry):
        slow_block(grid, pl.ds(pl.multiple_of(block * TURN, TURN), TURN))
        return carry

    slow_block(head, pl.ds(0, TURN))
    lax.fori_loop(1, count // TURN, slow_step, 0)

    def fast_step(number, carry):
        near = split_high[pl.ds(number * PAIR, PAIR)].reshape(PAIR * count, 2 * LANES)
        far = split_low[pl.ds(number * PAIR, PAIR)].reshape(PAIR * count, 2 * LANES)
        both = jnp.concatenate([near, near, far], axis=1)
        value = lax.dot_general(
            matrix[...], both, (((1,), (1,)), ((), ())), preferred_element_type=jnp.float32
        )
        level = jnp.abs(value) * scale[:1, :1] + FLOOR
        square = level * level
        sixth = square * level
        sixth = sixth * sixth
        level = sixth * sixth
        level = jnp.where(value < 0.0, -level, level)
        for part in range(2):
            for item in range(PAIR):
                rows[part, pl.ds(number * PAIR + item, LANES, stride=PITCH), :] = level[
                    part * LANES : (part + 1) * LANES, item * count : (item + 1) * count
                ]
        return carry

    lax.fori_loop(0, SLOW // PAIR, fast_step, 0, unroll=UNROLL)

    share = LANES // 8
    for d in range(8):
        first = jnp.bitwise_xor(me, d) * share * PITCH
        for part in range(2):
            for fast in range(share):
                start = pl.multiple_of(first + fast * PITCH, 4)
                pieces[d][pl.ds((part * share + fast) * SLOW, SLOW), :] = rows[
                    part, pl.ds(start, SLOW), :
                ].astype(jnp.bfloat16)
        pieces[d][pl.ds(2 * share * SLOW, 8), :] = scale.astype(jnp.bfloat16)


def encode(edge, taps, grid, largest, twist, matrix):
    count = grid.shape[2]
    channels = taps.shape[1]
    piece = jax.ShapeDtypeStruct((2 * channels // 8 + 8, count), jnp.bfloat16)
    whole = pl.BlockSpec(memory_space=pltpu.VMEM)
    return pl.pallas_call(
        encode_kernel,
        out_shape=[piece] * 8,
        in_specs=[whole] * 6,
        out_specs=[whole] * 8,
        scratch_shapes=[
            pltpu.VMEM((2 * LEAD, LANES), jnp.float32),
            pltpu.VMEM((2, SLOW, LEAD, LANES), jnp.float32),
            pltpu.VMEM((2, SLOW, TURN, LANES), jnp.float32),
            pltpu.VMEM((SLOW, count, 2 * LANES), jnp.bfloat16),
            pltpu.VMEM((SLOW, count, 2 * LANES), jnp.bfloat16),
            pltpu.VMEM((2, PITCH * LANES, LANES), jnp.float32),
        ],
        compiler_params=pltpu.CompilerParams(vmem_limit_bytes=20 * 1024 * 1024),
        name="encode",
    )(edge, taps, grid, largest, twist, matrix)


def decode_kernel(*rest):
    pieces = rest[:8]
    output = rest[-1]
    width = output.shape[2]
    half = (pieces[0].shape[0] - 8) // 2
    me = lax.axis_index("tm")
    base = pl.program_id(0) * width
    inverse = [1.0 / pieces[d][pl.ds(2 * half, 8), :].astype(jnp.float32) for d in range(8)]

    def step(number, carry):
        power = None
        found = []
        for d in range(8):
            for part in range(2):
                start = pl.multiple_of(part * half + base + number * 16, 16)
                code = pieces[d][pl.ds(start, 16), :].astype(jnp.float32)
                level = jnp.exp2(jnp.log2(jnp.abs(code)) * (1.0 / POWER)) - FLOOR
                level = level * inverse[d][:1]
                found.append(jnp.where(code < 0.0, -level, level))
                power = level * level if power is None else power + level * level
        total = jnp.sum(power, axis=1, keepdims=True)
        factor = lax.rsqrt(total / (8 * LANES) + 1.0)
        for d in range(8):
            lanes = pl.ds(pl.multiple_of(jnp.bitwise_xor(me, d) * LANES, LANES), LANES)
            for part in range(2):
                output[0, part, pl.ds(pl.multiple_of(number * 16, 16), 16), lanes] = found[2 * d + part] * factor
        return carry

    lax.fori_loop(0, width // 16, step, 0, unroll=8)


def decode(pieces, stream, streams, before):
    half = (pieces[0].shape[0] - 8) // 2
    blocks = 4
    shape = (streams, 2, half, 8 * LANES)
    whole = pl.BlockSpec(memory_space=pltpu.VMEM)
    operands = [*pieces]
    in_specs = [whole] * 8
    aliases = {}
    if before is not None:
        operands.append(before)
        in_specs.append(pl.BlockSpec(memory_space=pl.ANY))
        aliases = {8: 0}
    return pl.pallas_call(
        decode_kernel,
        grid=(blocks,),
        out_shape=jax.ShapeDtypeStruct(shape, jnp.float32),
        in_specs=in_specs,
        out_specs=pl.BlockSpec((1, 2, half // blocks, 8 * LANES), lambda i: (stream, 0, i, 0)),
        input_output_aliases=aliases,
        compiler_params=pltpu.CompilerParams(vmem_limit_bytes=16 * 1024 * 1024),
        name="decode",
    )(*operands)


def shards(signal, taps):
    streams = signal.shape[0]
    channels = taps.shape[1]
    count = signal.shape[2] // channels
    size = lax.axis_size("tm")
    twist, matrix = tables(channels)
    route = [(i, i + 1) for i in range(size - 1)]
    tails = [signal[s : s + 1, :, (count - LEAD) * channels :] for s in range(streams)]
    edge = lax.ppermute(tails[0], "tm", route)
    arrived = []
    held = signal
    for stream in range(streams):
        frames = held[stream].reshape(2, count, channels)
        grid, largest = filtered(frames, taps)
        near = edge.reshape(2, LEAD, channels)
        if stream + 1 < streams:
            tail, largest = lax.optimization_barrier((tails[stream + 1], largest))
            edge = lax.ppermute(tail, "tm", route)
        pieces = list(encode(near, taps, grid, largest, twist, matrix))
        held, pieces[0] = lax.optimization_barrier((held, pieces[0]))
        for d in ORDER:
            pieces[d] = lax.ppermute(pieces[d], "tm", [(i, i ^ d) for i in range(size)])
        arrived.append(pieces)
    output = None
    for stream in range(streams):
        output = decode(arrived[stream], stream, streams, output)
    return output


def solution(mesh):
    in_specs = (P("stream", None, "tm"), P())
    out_specs = P("stream", None, "tm", None)
    return jax.shard_map(shards, mesh=mesh, in_specs=in_specs, out_specs=out_specs, check_vma=False)
```

```python
import itertools
import math

import jax
import jax.numpy as jnp
import numpy as np
from jax import lax
from jax.experimental import pallas as pl
from jax.experimental.pallas import tpu as pltpu
from jax.sharding import PartitionSpec as P


SLOW = 32
LANES = 128
TURN = 16
LEAD = 16
PAIR = 4
UNROLL = 4
PITCH = 36
ORDER = ((0, 5, 1, 4, 7, 2, 3, 6), (0, 4, 5, 1, 2, 7, 6, 3))
POWER = 12
FLOOR = 2.0**-10.25
REACH = 2.0**10.25


def partner(slot):
    core = lax.axis_index("stream") % 2
    return ORDER[0][slot] + core * (ORDER[1][slot] - ORDER[0][slot])


def tables(channels):
    slow = np.arange(SLOW)[:, None]
    fast = np.arange(LANES)[None, :]
    angle = -2.0 * math.pi * slow * fast / channels
    twist = np.stack([np.cos(angle), np.sin(angle)]).astype(np.float32)
    turn = 2.0 * math.pi * (np.arange(LANES)[:, None] * fast % LANES) / LANES
    cosine, sine = np.cos(turn), np.sin(turn)
    matrix = np.block([[cosine, sine], [-sine, cosine]]) / math.sqrt(channels)
    high = matrix.astype(jnp.bfloat16)
    low = (matrix - high.astype(np.float64)).astype(jnp.bfloat16)
    return twist, np.concatenate([high, low, high], axis=1)


def turned(value, numerator, denominator):
    real, imag = value
    eighth = (8 * numerator) % (8 * denominator)
    if eighth % denominator == 0:
        step = eighth // denominator
        half = math.sqrt(0.5)
        return [
            lambda: (real, imag),
            lambda: ((real + imag) * half, (imag - real) * half),
            lambda: (imag, -real),
            lambda: ((imag - real) * half, (real + imag) * -half),
            lambda: (-real, -imag),
            lambda: ((real + imag) * -half, (real - imag) * half),
            lambda: (-imag, real),
            lambda: ((real - imag) * half, (real + imag) * half),
        ][step]()
    angle = -2.0 * math.pi * numerator / denominator
    cosine, sine = math.cos(angle), math.sin(angle)
    return (real * cosine - imag * sine, real * sine + imag * cosine)


def fourier(values):
    count = len(values)
    if count == 1:
        return values
    even = fourier(values[0::2])
    odd = fourier(values[1::2])
    odd = [turned(item, index, count) for index, item in enumerate(odd)]
    upper = [(a[0] + b[0], a[1] + b[1]) for a, b in zip(even, odd)]
    lower = [(a[0] - b[0], a[1] - b[1]) for a, b in zip(even, odd)]
    return upper + lower


def filter_kernel(frames, taps, grid, largest, window):
    depth = taps.shape[0]
    count = frames.shape[1]
    window[:, pl.ds(0, LEAD), :] = jnp.zeros((2, LEAD, LANES), jnp.float32)

    def step(slow, most):
        columns = pl.ds(pl.multiple_of(slow * LANES, LANES), LANES)
        weights = [taps[pl.ds(k, 1), columns] for k in range(depth)]
        for part in range(2):
            window[part, pl.ds(LEAD, count), :] = frames[part, :, columns].astype(jnp.float32)
        for part, block in itertools.product(range(2), range(count // 8)):
            total = None
            for k in range(depth):
                if 8 * block + 7 < k:
                    continue
                term = weights[k] * window[part, pl.ds(LEAD + block * 8 - k, 8), :]
                total = term if total is None else total + term
            grid[part, slow, pl.ds(block * 8, 8), :] = total
            most = jnp.maximum(most, jnp.abs(total))
        return most

    largest[...] = lax.fori_loop(0, SLOW, step, jnp.zeros((8, LANES), jnp.float32), unroll=2)


def filtered(frames, taps):
    count = frames.shape[1]
    whole = pl.BlockSpec(memory_space=pltpu.VMEM)
    return pl.pallas_call(
        filter_kernel,
        out_shape=[
            jax.ShapeDtypeStruct((2, SLOW, count, LANES), jnp.float32),
            jax.ShapeDtypeStruct((8, LANES), jnp.float32),
        ],
        in_specs=[whole] * 2,
        out_specs=[whole] * 2,
        scratch_shapes=[pltpu.VMEM((2, LEAD + count, LANES), jnp.float32)],
        compiler_params=pltpu.CompilerParams(vmem_limit_bytes=12 * 1024 * 1024),
        name="filter",
    )(frames, taps)


def encode_kernel(edge, taps, grid, largest, twist, matrix, *rest):
    pieces = rest[:8]
    window, head, half, split_high, split_low, rows = rest[8:]
    depth = taps.shape[0]
    count = grid.shape[2]
    me = lax.axis_index("tm")
    window[pl.ds(LEAD, LEAD), :] = jnp.zeros((LEAD, LANES), jnp.float32)

    def head_step(number, most):
        part = number // SLOW
        slow = number % SLOW
        columns = pl.ds(pl.multiple_of(slow * LANES, LANES), LANES)
        window[pl.ds(0, LEAD), :] = edge[part, :, columns].astype(jnp.float32)
        weights = [taps[pl.ds(k, 1), columns] for k in range(depth)]
        for block in range(LEAD // 8):
            times = pl.ds(block * 8, 8)
            total = grid[part, slow, times, :]
            for k in range(8 * block + 1, depth):
                total = total + weights[k] * window[pl.ds(LEAD + block * 8 - k, 8), :]
            head[part, slow, times, :] = total
            most = jnp.maximum(most, jnp.abs(total))
        return most

    most = lax.fori_loop(0, 2 * SLOW, head_step, largest[...], unroll=4)
    bound = jnp.max(most) * math.sqrt(2.0 * LANES * SLOW)
    scale = jnp.full((8, LANES), REACH, jnp.float32) / jnp.maximum(bound, 1e-35)
    scale = scale.astype(jnp.bfloat16).astype(jnp.float32)

    def slow_block(source, times):
        for j in range(4):
            column = [(source[0, 4 * i + j, times, :], source[1, 4 * i + j, times, :]) for i in range(8)]
            for u, item in enumerate(fourier(column)):
                real, imag = turned(item, j * u, SLOW)
                half[0, 4 * u + j] = real
                half[1, 4 * u + j] = imag
        for u in range(8):
            column = [(half[0, 4 * u + j], half[1, 4 * u + j]) for j in range(4)]
            for w, (real, imag) in enumerate(fourier(column)):
                slow = u + 8 * w
                cosine = twist[0, pl.ds(slow, 1), :]
                sine = twist[1, pl.ds(slow, 1), :]
                for part, value in enumerate((real * cosine - imag * sine, real * sine + imag * cosine)):
                    top = value.astype(jnp.bfloat16)
                    lanes = pl.ds(part * LANES, LANES)
                    split_high[slow, times, lanes] = top
                    split_low[slow, times, lanes] = (value - top.astype(jnp.float32)).astype(jnp.bfloat16)

    def slow_step(block, carry):
        slow_block(grid, pl.ds(pl.multiple_of(block * TURN, TURN), TURN))
        return carry

    slow_block(head, pl.ds(0, TURN))
    lax.fori_loop(1, count // TURN, slow_step, 0)

    def fast_step(number, carry):
        near = split_high[pl.ds(number * PAIR, PAIR)].reshape(PAIR * count, 2 * LANES)
        far = split_low[pl.ds(number * PAIR, PAIR)].reshape(PAIR * count, 2 * LANES)
        both = jnp.concatenate([near, near, far], axis=1)
        value = lax.dot_general(
            matrix[...], both, (((1,), (1,)), ((), ())), preferred_element_type=jnp.float32
        )
        level = jnp.abs(value) * scale[:1, :1] + FLOOR
        square = level * level
        sixth = square * level
        sixth = sixth * sixth
        level = sixth * sixth
        level = jnp.where(value < 0.0, -level, level)
        for part in range(2):
            for item in range(PAIR):
                rows[part, pl.ds(number * PAIR + item, LANES, stride=PITCH), :] = level[
                    part * LANES : (part + 1) * LANES, item * count : (item + 1) * count
                ]
        return carry

    lax.fori_loop(0, SLOW // PAIR, fast_step, 0, unroll=UNROLL)

    share = LANES // 8
    for d in range(8):
        first = jnp.bitwise_xor(me, partner(d)) * share * PITCH
        for part in range(2):
            for fast in range(share):
                start = pl.multiple_of(first + fast * PITCH, 4)
                pieces[d][pl.ds((part * share + fast) * SLOW, SLOW), :] = rows[
                    part, pl.ds(start, SLOW), :
                ].astype(jnp.bfloat16)
        pieces[d][pl.ds(2 * share * SLOW, 8), :] = scale.astype(jnp.bfloat16)


def encode(edge, taps, grid, largest, twist, matrix):
    count = grid.shape[2]
    channels = taps.shape[1]
    piece = jax.ShapeDtypeStruct((2 * channels // 8 + 8, count), jnp.bfloat16)
    whole = pl.BlockSpec(memory_space=pltpu.VMEM)
    return pl.pallas_call(
        encode_kernel,
        out_shape=[piece] * 8,
        in_specs=[whole] * 6,
        out_specs=[whole] * 8,
        scratch_shapes=[
            pltpu.VMEM((2 * LEAD, LANES), jnp.float32),
            pltpu.VMEM((2, SLOW, LEAD, LANES), jnp.float32),
            pltpu.VMEM((2, SLOW, TURN, LANES), jnp.float32),
            pltpu.VMEM((SLOW, count, 2 * LANES), jnp.bfloat16),
            pltpu.VMEM((SLOW, count, 2 * LANES), jnp.bfloat16),
            pltpu.VMEM((2, PITCH * LANES, LANES), jnp.float32),
        ],
        compiler_params=pltpu.CompilerParams(vmem_limit_bytes=20 * 1024 * 1024),
        name="encode",
    )(edge, taps, grid, largest, twist, matrix)


def decode_kernel(*rest):
    pieces = rest[:8]
    output = rest[-1]
    width = output.shape[2]
    half = (pieces[0].shape[0] - 8) // 2
    me = lax.axis_index("tm")
    base = pl.program_id(0) * width
    inverse = [1.0 / pieces[d][pl.ds(2 * half, 8), :].astype(jnp.float32) for d in range(8)]

    def step(number, carry):
        power = None
        found = []
        for d in range(8):
            for part in range(2):
                start = pl.multiple_of(part * half + base + number * 16, 16)
                code = pieces[d][pl.ds(start, 16), :].astype(jnp.float32)
                level = jnp.exp2(jnp.log2(jnp.abs(code)) * (1.0 / POWER)) - FLOOR
                level = level * inverse[d][:1]
                found.append(jnp.where(code < 0.0, -level, level))
                power = level * level if power is None else power + level * level
        total = jnp.sum(power, axis=1, keepdims=True)
        factor = lax.rsqrt(total / (8 * LANES) + 1.0)
        for d in range(8):
            lanes = pl.ds(pl.multiple_of(jnp.bitwise_xor(me, partner(d)) * LANES, LANES), LANES)
            for part in range(2):
                output[0, part, pl.ds(pl.multiple_of(number * 16, 16), 16), lanes] = found[2 * d + part] * factor
        return carry

    lax.fori_loop(0, width // 16, step, 0, unroll=8)


def decode(pieces, stream, streams, before):
    half = (pieces[0].shape[0] - 8) // 2
    blocks = 4
    shape = (streams, 2, half, 8 * LANES)
    whole = pl.BlockSpec(memory_space=pltpu.VMEM)
    operands = [*pieces]
    in_specs = [whole] * 8
    aliases = {}
    if before is not None:
        operands.append(before)
        in_specs.append(pl.BlockSpec(memory_space=pl.ANY))
        aliases = {8: 0}
    return pl.pallas_call(
        decode_kernel,
        grid=(blocks,),
        out_shape=jax.ShapeDtypeStruct(shape, jnp.float32),
        in_specs=in_specs,
        out_specs=pl.BlockSpec((1, 2, half // blocks, 8 * LANES), lambda i: (stream, 0, i, 0)),
        input_output_aliases=aliases,
        compiler_params=pltpu.CompilerParams(vmem_limit_bytes=16 * 1024 * 1024),
        name="decode",
    )(*operands)


def shards(signal, taps):
    streams = signal.shape[0]
    channels = taps.shape[1]
    count = signal.shape[2] // channels
    size = lax.axis_size("tm")
    twist, matrix = tables(channels)
    route = [(i, i + 1) for i in range(size - 1)]
    tails = [signal[s : s + 1, :, (count - LEAD) * channels :] for s in range(streams)]
    edge = lax.ppermute(tails[0], "tm", route)
    arrived = []
    held = signal
    for stream in range(streams):
        frames = held[stream].reshape(2, count, channels)
        grid, largest = filtered(frames, taps)
        near = edge.reshape(2, LEAD, channels)
        if stream + 1 < streams:
            tail, largest = lax.optimization_barrier((tails[stream + 1], largest))
            edge = lax.ppermute(tail, "tm", route)
        pieces = list(encode(near, taps, grid, largest, twist, matrix))
        held, pieces[0] = lax.optimization_barrier((held, pieces[0]))
        for slot in range(1, size):
            ways = [
                (row * size + i, row * size + (i ^ ORDER[row % 2][slot]))
                for row in range(lax.axis_size("stream"))
                for i in range(size)
            ]
            pieces[slot] = lax.ppermute(pieces[slot], ("stream", "tm"), ways)
        arrived.append(pieces)
    output = None
    for stream in range(streams):
        output = decode(arrived[stream], stream, streams, output)
    return output


def solution(mesh):
    in_specs = (P("stream", None, "tm"), P())
    out_specs = P("stream", None, "tm", None)
    return jax.shard_map(shards, mesh=mesh, in_specs=in_specs, out_specs=out_specs, check_vma=False)
```

```python
import itertools
import math

import jax
import jax.numpy as jnp
import numpy as np
from jax import lax
from jax.experimental import pallas as pl
from jax.experimental.pallas import tpu as pltpu
from jax.sharding import PartitionSpec as P


SLOW = 32
LANES = 128
TURN = 16
LEAD = 16
PAIR = 4
UNROLL = 8
PITCH = 36
ORDER = (1, 5, 4, 7, 2, 3, 6)
POWER = 12
FLOOR = 2.0**-10.25
REACH = 2.0**10.25


def tables(channels):
    slow = np.arange(SLOW)[:, None]
    fast = np.arange(LANES)[None, :]
    angle = -2.0 * math.pi * slow * fast / channels
    twist = np.stack([np.cos(angle), np.sin(angle)]).astype(np.float32)
    turn = 2.0 * math.pi * (np.arange(LANES)[:, None] * fast % LANES) / LANES
    cosine, sine = np.cos(turn), np.sin(turn)
    matrix = np.block([[cosine, sine], [-sine, cosine]]) / math.sqrt(channels)
    high = matrix.astype(jnp.bfloat16)
    low = (matrix - high.astype(np.float64)).astype(jnp.bfloat16)
    return twist, np.concatenate([high, low, high], axis=1)


def turned(value, numerator, denominator):
    real, imag = value
    eighth = (8 * numerator) % (8 * denominator)
    if eighth % denominator == 0:
        step = eighth // denominator
        half = math.sqrt(0.5)
        return [
            lambda: (real, imag),
            lambda: ((real + imag) * half, (imag - real) * half),
            lambda: (imag, -real),
            lambda: ((imag - real) * half, (real + imag) * -half),
            lambda: (-real, -imag),
            lambda: ((real + imag) * -half, (real - imag) * half),
            lambda: (-imag, real),
            lambda: ((real - imag) * half, (real + imag) * half),
        ][step]()
    angle = -2.0 * math.pi * numerator / denominator
    cosine, sine = math.cos(angle), math.sin(angle)
    return (real * cosine - imag * sine, real * sine + imag * cosine)


def fourier(values):
    count = len(values)
    if count == 1:
        return values
    even = fourier(values[0::2])
    odd = fourier(values[1::2])
    odd = [turned(item, index, count) for index, item in enumerate(odd)]
    upper = [(a[0] + b[0], a[1] + b[1]) for a, b in zip(even, odd)]
    lower = [(a[0] - b[0], a[1] - b[1]) for a, b in zip(even, odd)]
    return upper + lower


def filter_kernel(frames, taps, grid, largest, window):
    depth = taps.shape[0]
    count = frames.shape[1]
    window[:, pl.ds(0, LEAD), :] = jnp.zeros((2, LEAD, LANES), jnp.float32)

    def step(slow, most):
        columns = pl.ds(pl.multiple_of(slow * LANES, LANES), LANES)
        weights = [taps[pl.ds(k, 1), columns] for k in range(depth)]
        for part in range(2):
            window[part, pl.ds(LEAD, count), :] = frames[part, :, columns].astype(jnp.float32)
        for part, block in itertools.product(range(2), range(count // 8)):
            total = None
            for k in range(depth):
                if 8 * block + 7 < k:
                    continue
                term = weights[k] * window[part, pl.ds(LEAD + block * 8 - k, 8), :]
                total = term if total is None else total + term
            grid[part, slow, pl.ds(block * 8, 8), :] = total
            most = jnp.maximum(most, jnp.abs(total))
        return most

    largest[...] = lax.fori_loop(0, SLOW, step, jnp.zeros((8, LANES), jnp.float32), unroll=2)


def filtered(frames, taps):
    count = frames.shape[1]
    whole = pl.BlockSpec(memory_space=pltpu.VMEM)
    return pl.pallas_call(
        filter_kernel,
        out_shape=[
            jax.ShapeDtypeStruct((2, SLOW, count, LANES), jnp.float32),
            jax.ShapeDtypeStruct((8, LANES), jnp.float32),
        ],
        in_specs=[whole] * 2,
        out_specs=[whole] * 2,
        scratch_shapes=[pltpu.VMEM((2, LEAD + count, LANES), jnp.float32)],
        compiler_params=pltpu.CompilerParams(vmem_limit_bytes=12 * 1024 * 1024),
        name="filter",
    )(frames, taps)


def encode_kernel(edge, taps, grid, largest, twist, matrix, *rest):
    pieces = rest[:8]
    window, head, half, split_high, split_low, rows = rest[8:]
    depth = taps.shape[0]
    count = grid.shape[2]
    me = lax.axis_index("tm")
    window[:, pl.ds(LEAD, LEAD), :] = jnp.zeros((2, LEAD, LANES), jnp.float32)

    def head_step(slow, most):
        columns = pl.ds(pl.multiple_of(slow * LANES, LANES), LANES)
        weights = [taps[pl.ds(k, 1), columns] for k in range(depth)]
        for part in range(2):
            window[part, pl.ds(0, LEAD), :] = edge[part, :, columns].astype(jnp.float32)
            for block in range(LEAD // 8):
                times = pl.ds(block * 8, 8)
                total = grid[part, slow, times, :]
                for k in range(8 * block + 1, depth):
                    total = total + weights[k] * window[part, pl.ds(LEAD + block * 8 - k, 8), :]
                head[part, slow, times, :] = total
                most = jnp.maximum(most, jnp.abs(total))
        return most

    most = lax.fori_loop(0, SLOW, head_step, largest[...], unroll=4)
    bound = jnp.max(most) * math.sqrt(2.0 * LANES * SLOW)
    scale = jnp.full((8, LANES), REACH, jnp.float32) / jnp.maximum(bound, 1e-35)
    scale = scale.astype(jnp.bfloat16).astype(jnp.float32)

    def slow_block(source, times):
        for j in range(4):
            column = [(source[0, 4 * i + j, times, :], source[1, 4 * i + j, times, :]) for i in range(8)]
            for u, item in enumerate(fourier(column)):
                real, imag = turned(item, j * u, SLOW)
                half[0, 4 * u + j] = real
                half[1, 4 * u + j] = imag
        for u in range(8):
            column = [(half[0, 4 * u + j], half[1, 4 * u + j]) for j in range(4)]
            for w, (real, imag) in enumerate(fourier(column)):
                slow = u + 8 * w
                cosine = twist[0, pl.ds(slow, 1), :]
                sine = twist[1, pl.ds(slow, 1), :]
                for part, value in enumerate((real * cosine - imag * sine, real * sine + imag * cosine)):
                    top = value.astype(jnp.bfloat16)
                    lanes = pl.ds(part * LANES, LANES)
                    split_high[slow, times, lanes] = top
                    split_low[slow, times, lanes] = (value - top.astype(jnp.float32)).astype(jnp.bfloat16)

    def slow_step(block, carry):
        slow_block(grid, pl.ds(pl.multiple_of(block * TURN, TURN), TURN))
        return carry

    slow_block(head, pl.ds(0, TURN))
    lax.fori_loop(1, count // TURN, slow_step, 0)

    def fast_step(number, carry):
        near = split_high[pl.ds(number * PAIR, PAIR)].reshape(PAIR * count, 2 * LANES)
        far = split_low[pl.ds(number * PAIR, PAIR)].reshape(PAIR * count, 2 * LANES)
        both = jnp.concatenate([near, near, far], axis=1)
        value = lax.dot_general(
            matrix[...], both, (((1,), (1,)), ((), ())), preferred_element_type=jnp.float32
        )
        level = jnp.abs(value) * scale[:1, :1] + FLOOR
        square = level * level
        sixth = square * level
        sixth = sixth * sixth
        level = sixth * sixth
        level = jnp.where(value < 0.0, -level, level)
        for part in range(2):
            for item in range(PAIR):
                rows[part, pl.ds(number * PAIR + item, LANES, stride=PITCH), :] = level[
                    part * LANES : (part + 1) * LANES, item * count : (item + 1) * count
                ]
        return carry

    lax.fori_loop(0, SLOW // PAIR, fast_step, 0, unroll=UNROLL)

    share = LANES // 8
    for d in range(8):
        first = jnp.bitwise_xor(me, d) * share * PITCH
        for part in range(2):
            for fast in range(share):
                start = pl.multiple_of(first + fast * PITCH, 4)
                pieces[d][pl.ds((part * share + fast) * SLOW, SLOW), :] = rows[
                    part, pl.ds(start, SLOW), :
                ].astype(jnp.bfloat16)
        pieces[d][pl.ds(2 * share * SLOW, 8), :] = scale.astype(jnp.bfloat16)


def encode(edge, taps, grid, largest, twist, matrix):
    count = grid.shape[2]
    channels = taps.shape[1]
    piece = jax.ShapeDtypeStruct((2 * channels // 8 + 8, count), jnp.bfloat16)
    whole = pl.BlockSpec(memory_space=pltpu.VMEM)
    return pl.pallas_call(
        encode_kernel,
        out_shape=[piece] * 8,
        in_specs=[whole] * 6,
        out_specs=[whole] * 8,
        scratch_shapes=[
            pltpu.VMEM((2, 2 * LEAD, LANES), jnp.float32),
            pltpu.VMEM((2, SLOW, LEAD, LANES), jnp.float32),
            pltpu.VMEM((2, SLOW, TURN, LANES), jnp.float32),
            pltpu.VMEM((SLOW, count, 2 * LANES), jnp.bfloat16),
            pltpu.VMEM((SLOW, count, 2 * LANES), jnp.bfloat16),
            pltpu.VMEM((2, PITCH * LANES, LANES), jnp.float32),
        ],
        compiler_params=pltpu.CompilerParams(vmem_limit_bytes=20 * 1024 * 1024),
        name="encode",
    )(edge, taps, grid, largest, twist, matrix)


def decode_kernel(*rest):
    pieces = rest[:8]
    output = rest[-1]
    width = output.shape[2]
    half = (pieces[0].shape[0] - 8) // 2
    me = lax.axis_index("tm")
    base = pl.program_id(0) * width
    inverse = [1.0 / pieces[d][pl.ds(2 * half, 8), :].astype(jnp.float32) for d in range(8)]

    def step(number, carry):
        power = None
        found = []
        for d in range(8):
            for part in range(2):
                start = pl.multiple_of(part * half + base + number * 16, 16)
                code = pieces[d][pl.ds(start, 16), :].astype(jnp.float32)
                level = jnp.exp2(jnp.log2(jnp.abs(code)) * (1.0 / POWER)) - FLOOR
                level = level * inverse[d][:1]
                found.append(jnp.where(code < 0.0, -level, level))
                power = level * level if power is None else power + level * level
        total = jnp.sum(power, axis=1, keepdims=True)
        factor = lax.rsqrt(total / (8 * LANES) + 1.0)
        for d in range(8):
            lanes = pl.ds(pl.multiple_of(jnp.bitwise_xor(me, d) * LANES, LANES), LANES)
            for part in range(2):
                output[0, part, pl.ds(pl.multiple_of(number * 16, 16), 16), lanes] = found[2 * d + part] * factor
        return carry

    lax.fori_loop(0, width // 16, step, 0, unroll=8)


def decode(pieces, stream, streams, before):
    half = (pieces[0].shape[0] - 8) // 2
    blocks = 4
    shape = (streams, 2, half, 8 * LANES)
    whole = pl.BlockSpec(memory_space=pltpu.VMEM)
    operands = [*pieces]
    in_specs = [whole] * 8
    aliases = {}
    if before is not None:
        operands.append(before)
        in_specs.append(pl.BlockSpec(memory_space=pl.ANY))
        aliases = {8: 0}
    return pl.pallas_call(
        decode_kernel,
        grid=(blocks,),
        out_shape=jax.ShapeDtypeStruct(shape, jnp.float32),
        in_specs=in_specs,
        out_specs=pl.BlockSpec((1, 2, half // blocks, 8 * LANES), lambda i: (stream, 0, i, 0)),
        input_output_aliases=aliases,
        compiler_params=pltpu.CompilerParams(vmem_limit_bytes=16 * 1024 * 1024),
        name="decode",
    )(*operands)


def shards(signal, taps):
    streams = signal.shape[0]
    channels = taps.shape[1]
    count = signal.shape[2] // channels
    size = lax.axis_size("tm")
    twist, matrix = tables(channels)
    route = [(i, i + 1) for i in range(size - 1)]
    tails = [signal[s : s + 1, :, (count - LEAD) * channels :] for s in range(streams)]
    edge = lax.ppermute(tails[0], "tm", route)
    arrived = []
    held = signal
    for stream in range(streams):
        frames = held[stream].reshape(2, count, channels)
        grid, largest = filtered(frames, taps)
        near = edge.reshape(2, LEAD, channels)
        if stream + 1 < streams:
            tail, largest = lax.optimization_barrier((tails[stream + 1], largest))
            edge = lax.ppermute(tail, "tm", route)
        pieces = list(encode(near, taps, grid, largest, twist, matrix))
        held, pieces[0] = lax.optimization_barrier((held, pieces[0]))
        for d in ORDER:
            pieces[d] = lax.ppermute(pieces[d], "tm", [(i, i ^ d) for i in range(size)])
        arrived.append(pieces)
    output = None
    for stream in range(streams):
        output = decode(arrived[stream], stream, streams, output)
    return output


def solution(mesh):
    in_specs = (P("stream", None, "tm"), P())
    out_specs = P("stream", None, "tm", None)
    return jax.shard_map(shards, mesh=mesh, in_specs=in_specs, out_specs=out_specs, check_vma=False)
```
